8 devices in a mesh: dp: 2 (over y, z), tp: 4 (over x, core).
Axes of the slice: x: 2, y: 2, z: 1, core: 2. Of those that a mesh axis runs over, the one named last changes fastest.
Arguments:
- x: bfloat16 [4096, 3072], P('dp'), parts along dimension 0
- dy: bfloat16 [4096, 3072], P('dp'), parts along dimension 0
- gate: bfloat16 [4096, 8192], P('dp', 'tp'), parts along dimension 0
- up: bfloat16 [4096, 8192], P('dp', 'tp'), parts along dimension 0
- w_gate: bfloat16 [3072, 8192], P(None, 'tp')
- w_up: bfloat16 [3072, 8192], P(None, 'tp')
- w_down: bfloat16 [8192, 3072], P('tp')
Outputs:
- output 1: bfloat16 [4096, 3072], P('dp'), parts along dimension 0
- output 2: bfloat16 [6144, 8192], P('dp', 'tp'), parts along dimension 0
- output 3: bfloat16 [6144, 8192], P('dp', 'tp'), parts along dimension 0
- output 4: bfloat16 [16384, 3072], P(('dp', 'tp')), parts along dimension 0
There are 2 independent parts. The reference program is written for one: setup_inputs(seed, part) draws one part's arguments, and reference() takes and returns one part's arrays. A program takes and returns all parts, laid end to end along the dimension named above; an argument that names none is the same for every part.
All inputs are finite; a program needn't handle non-finite values.
Results may differ from the reference program's by a relative error of at most 0.012.
Values are sent between devices in bfloat16 or wider.
A program may use at most 2 GiB of HBM per device.

```python
import jax
import jax.numpy as jnp

ROWS = 2048
D = 3072
FF = 8192


def act(gate, up):
    return jax.nn.silu(gate) * up


def setup_inputs(seed: int = 0, part: int = 0) -> dict:
    kx, ky, ka, kb, kg, ku, kd = jax.random.split(jax.random.key(seed), 7)
    kx, ky, ka, kb = (jax.random.fold_in(k, part) for k in (kx, ky, ka, kb))
    drawn = {
        "x": jax.random.normal(kx, (ROWS, D), jnp.float32),
        "dy": jax.random.normal(ky, (ROWS, D), jnp.float32),
        "gate": jax.random.normal(ka, (ROWS, FF), jnp.float32),
        "up": jax.random.normal(kb, (ROWS, FF), jnp.float32),
        "w_gate": jax.random.normal(kg, (D, FF), jnp.float32) * D**-0.5,
        "w_up": jax.random.normal(ku, (D, FF), jnp.float32) * D**-0.5,
        "w_down": jax.random.normal(kd, (FF, D), jnp.float32) * FF**-0.5,
    }
    return {k: v.astype(jnp.bfloat16) for k, v in drawn.items()}


def reference(x, dy, gate, up, w_gate, w_up, w_down):
    hidden, back = jax.vjp(act, gate.astype(jnp.float32), up.astype(jnp.float32))
    d_hidden = jnp.dot(dy, w_down.T, preferred_element_type=jnp.float32)
    d_gate, d_up = (g.astype(jnp.bfloat16) for g in back(d_hidden))
    dx = jnp.dot(d_gate, w_gate.T, preferred_element_type=jnp.float32) + jnp.dot(d_up, w_up.T, preferred_element_type=jnp.float32)
    dw_gate = jnp.dot(x.T, d_gate, preferred_element_type=jnp.float32)
    dw_up = jnp.dot(x.T, d_up, preferred_element_type=jnp.float32)
    dw_down = jnp.dot(hidden.astype(jnp.bfloat16).T, dy, preferred_element_type=jnp.float32)
    return tuple(g.astype(jnp.bfloat16) for g in (dx, dw_gate, dw_up, dw_down))
```

```python
import jax
import jax.numpy as jnp
from jax import lax
from jax.experimental import pallas as pl
from jax.experimental.pallas import tpu as pltpu
from jax.sharding import PartitionSpec as P

NT = (((1,), (1,)), ((), ()))
TN = (((0,), (0,)), ((), ()))
MESH = pl.DeviceIdType.MESH
VMEM_LIMIT = 64 * 1024 * 1024 - 65536
BF = jnp.bfloat16
ROWS = 256
HALF = ROWS // 2
WIDE = 512


def dot(a, b, dims):
    return lax.dot_general(a, b, dims, preferred_element_type=jnp.float32)


def kernel(
    x, dy, gate, up, wg, wu, wd,
    dxt, dwg, dwu, hid, dgu,
    wd_v, w_v, dy_v, g_v, u_v, dgu_v, h_v, term_v, s_v, q_v, blk_v,
    wd_sem, w_sem, in_sem, out_sem, x_sem, blk_sem, o_sem,
    give_send, give_recv, link_send, link_recv, fin_local, fin_send, fin_recv,
):
    tokens, d = x.shape
    ff = gate.shape[1]
    chunks = tokens // ROWS
    me = lax.axis_index("tp")
    core = lax.rem(me, 2)
    mate = {"tp": me + 1 - 2 * core}
    across = {"tp": lax.rem(me + 2, 4)}
    own = pl.ds(pl.multiple_of(core * HALF, HALF), HALF)
    other = pl.ds(pl.multiple_of((1 - core) * HALF, HALF), HALF)

    def rows_of(c):
        return pl.ds(pl.multiple_of(c * ROWS, ROWS), ROWS)

    def inputs(c):
        r = rows_of(c)
        return (
            pltpu.make_async_copy(dy.at[r, :], dy_v, in_sem.at[0]),
            pltpu.make_async_copy(gate.at[r, :], g_v, in_sem.at[1]),
            pltpu.make_async_copy(up.at[r, :], u_v, in_sem.at[2]),
        )

    def outputs(c):
        r = rows_of(c)
        return (
            pltpu.make_async_copy(dgu_v, dgu.at[r, :], out_sem.at[0]),
            pltpu.make_async_copy(h_v, hid.at[r, :], out_sem.at[1]),
        )

    def wd_piece(j):
        r = pl.ds(j * WIDE, WIDE)
        return pltpu.make_async_copy(wd.at[r, :], wd_v.at[r, :], wd_sem.at[j])

    def w_piece(j):
        r = pl.ds(j * WIDE, WIDE)
        return (
            pltpu.make_async_copy(wg.at[r, :], w_v.at[r, pl.ds(0, ff)], w_sem.at[0, j]),
            pltpu.make_async_copy(wu.at[r, :], w_v.at[r, pl.ds(ff, ff)], w_sem.at[1, j]),
        )

    def give(c):
        return pltpu.make_async_remote_copy(
            term_v.at[other, :], s_v.at[c], give_send.at[c], give_recv.at[c], device_id=mate, device_id_type=MESH
        )

    def link(c):
        return pltpu.make_async_remote_copy(
            s_v.at[c], q_v.at[c], link_send.at[c], link_recv.at[c], device_id=across, device_id_type=MESH
        )

    def final_rows(c):
        return dxt.at[pl.ds(pl.multiple_of(c * ROWS + core * HALF, HALF), HALF), :]

    def fin_here(c):
        return pltpu.make_async_copy(q_v.at[c], final_rows(c), fin_local.at[c])

    def fin_mate(c):
        return pltpu.make_async_remote_copy(
            q_v.at[c], final_rows(c), fin_send.at[c], fin_recv.at[c], device_id=mate, device_id_type=MESH
        )

    def add_term(c):
        give(c).wait_recv()

        def body(i, _):
            r = pl.ds(pl.multiple_of(i * 16, 16), 16)
            mine = term_v[pl.ds(pl.multiple_of(core * HALF + i * 16, 16), 16), :]
            s_v[c, r, :] = (s_v[c, r, :].astype(jnp.float32) + mine.astype(jnp.float32)).astype(BF)
            return 0

        lax.fori_loop(0, HALF // 16, body, 0)
        link(c).start()
        give(c).wait_send()

    def finish(c):
        link(c).wait_recv()

        def body(i, _):
            r = pl.ds(pl.multiple_of(i * 16, 16), 16)
            q_v[c, r, :] = (q_v[c, r, :].astype(jnp.float32) + s_v[c, r, :].astype(jnp.float32)).astype(BF)
            return 0

        lax.fori_loop(0, HALF // 16, body, 0)
        fin_here(c).start()
        fin_mate(c).start()

    def hidden_tile(j):
        cols = pl.ds(j * WIDE, WIDE)
        dh = dot(dy_v[...], wd_v[cols, :], NT)
        g = g_v[:, cols].astype(jnp.float32)
        u = u_v[:, cols].astype(jnp.float32)
        sig = 1.0 / (1.0 + jnp.exp(-g))
        silu = g * sig
        h_v[:, cols] = (silu * u).astype(BF)
        dgu_v[:, pl.ds(ff + j * WIDE, WIDE)] = (dh * silu).astype(BF)
        dgu_v[:, cols] = (dh * u * (sig + silu * (1.0 - sig))).astype(BF)

    def term_tile(j):
        cols = pl.ds(j * WIDE, WIDE)
        term_v[:, cols] = dot(dgu_v[...], w_v[cols, :], NT).astype(BF)

    n_h, n_t = ff // WIDE, d // WIDE

    for cp in inputs(0):
        cp.start()
    for j in range(n_h):
        wd_piece(j).start()
    for j in range(n_t):
        for cp in w_piece(j):
            cp.start()
    barrier = pltpu.get_barrier_semaphore()
    for peer in (mate, across):
        pl.semaphore_signal(barrier, inc=1, device_id=peer, device_id_type=MESH)
    for cp in inputs(0):
        cp.wait()
    for j in range(n_h):
        wd_piece(j).wait()
        hidden_tile(j)
    for cp in inputs(1):
        cp.start()
    for cp in outputs(0):
        cp.start()
    for j in range(n_t):
        for cp in w_piece(j):
            cp.wait()
        term_tile(j)
    pl.semaphore_wait(barrier, 2)
    give(0).start()

    def chunk(c, _):
        for cp in inputs(c):
            cp.wait()
        for cp in outputs(c - 1):
            cp.wait()
        for j in range(n_h // 2):
            hidden_tile(j)
        add_term(c - 1)
        for j in range(n_h // 2, n_h):
            hidden_tile(j)

        @pl.when(c < chunks - 1)
        def _():
            for cp in inputs(c + 1):
                cp.start()

        @pl.when(c == chunks - 1)
        def _():
            pltpu.make_async_copy(x, wd_v, x_sem).start()

        for cp in outputs(c):
            cp.start()

        @pl.when(c >= 5)
        def _():
            finish(c - 5)

        for j in range(n_t):
            term_tile(j)
        give(c).start()
        return 0

    lax.fori_loop(1, chunks, chunk, 0)

    def block(b, slot):
        return pltpu.make_async_copy(
            dgu.at[:, pl.ds(pl.multiple_of(b * WIDE, WIDE), WIDE)], blk_v.at[slot], blk_sem.at[slot]
        )

    tall = 1024
    n_m = d // tall
    n_b = ff // WIDE

    def stage(m):
        return w_v.at[pl.ds(m * tall, tall), pl.ds(0, WIDE)]

    def store(m, out, b):
        return pltpu.make_async_copy(
            stage(m), out.at[pl.ds(m * tall, tall), pl.ds(pl.multiple_of(b * WIDE, WIDE), WIDE)], o_sem.at[m]
        )

    for cp in outputs(chunks - 1):
        cp.wait()
    block(0, 0).start()
    block(1, 1).start()
    pltpu.make_async_copy(x, wd_v, x_sem).wait()

    def column_block(b, _):
        slot = lax.rem(b, 2)

        @pl.when(b == 0)
        def _():
            finish(3)

        @pl.when(b == 1)
        def _():
            add_term(chunks - 1)

        @pl.when(b == 2)
        def _():
            finish(4)

        @pl.when(b == 5)
        def _():
            finish(5)

        @pl.when(b == 7)
        def _():
            finish(6)

        @pl.when(b > 0)
        def _():
            for m in range(n_m):
                store(m, dwg, 0).wait()

        block(b, slot).wait()
        for m in range(n_m):
            w_v[m * tall:(m + 1) * tall, 0:WIDE] = dot(
                wd_v[:, m * tall:(m + 1) * tall], blk_v[slot], TN
            ).astype(BF)

        @pl.when(b < n_b)
        def _():
            for m in range(n_m):
                store(m, dwg, b).start()

        @pl.when(b >= n_b)
        def _():
            for m in range(n_m):
                store(m, dwu, b - n_b).start()

        @pl.when(b < 2 * n_b - 2)
        def _():
            block(b + 2, slot).start()

        return 0

    lax.fori_loop(0, 2 * n_b, column_block, 0)
    finish(chunks - 1)
    for m in range(n_m):
        store(m, dwg, 0).wait()
    for c in range(chunks):
        link(c).wait_send()
        fin_here(c).wait()
        fin_mate(c).wait()


def solution(mesh):
    def step(x, dy, gate, up, w_gate, w_up, w_down):
        tokens, d = x.shape
        ff = gate.shape[1]
        chunks = tokens // ROWS
        hbm = pl.BlockSpec(memory_space=pl.ANY)
        dma = pltpu.SemaphoreType.DMA
        dxt, dwg, dwu, hid, _ = pl.pallas_call(
            kernel,
            name="chunks",
            in_specs=[hbm] * 7,
            out_specs=[hbm] * 5,
            out_shape=[
                jax.ShapeDtypeStruct((tokens, d), BF),
                jax.ShapeDtypeStruct((d, ff), BF),
                jax.ShapeDtypeStruct((d, ff), BF),
                jax.ShapeDtypeStruct((tokens, ff), BF),
                jax.ShapeDtypeStruct((tokens, 2 * ff), BF),
            ],
            scratch_shapes=[
                pltpu.VMEM((ff, d), BF),
                pltpu.VMEM((d, 2 * ff), BF),
                pltpu.VMEM((ROWS, d), BF),
                pltpu.VMEM((ROWS, ff), BF),
                pltpu.VMEM((ROWS, ff), BF),
                pltpu.VMEM((ROWS, 2 * ff), BF),
                pltpu.VMEM((ROWS, ff), BF),
                pltpu.VMEM((ROWS, d), BF),
                pltpu.VMEM((chunks, HALF, d), BF),
                pltpu.VMEM((chunks, HALF, d), BF),
                pltpu.VMEM((2, tokens, WIDE), BF),
                dma((ff // WIDE,)),
                dma((2, d // WIDE)),
                dma((3,)),
                dma((2,)),
                dma,
                dma((2,)),
                dma((d // 1024,)),
            ]
            + [dma((chunks,))] * 7,
            compiler_params=pltpu.CompilerParams(
                collective_id=0, has_side_effects=True, vmem_limit_bytes=VMEM_LIMIT
            ),
        )(x, dy, gate, up, w_gate, w_up, w_down)
        dw_down = dot(hid, dy, TN).astype(BF)
        return dxt, dwg, dwu, dw_down

    tokens, columns, rows = P("dp", None), P(None, "tp"), P("tp", None)
    return jax.shard_map(
        step,
        mesh=mesh,
        in_specs=(tokens, tokens, P("dp", "tp"), P("dp", "tp"), columns, columns, rows),
        out_specs=(tokens, P("dp", "tp"), P("dp", "tp"), P(("dp", "tp"), None)),
        check_vma=False,
    )
```

```python
import jax
import jax.numpy as jnp
from jax import lax
from jax.experimental import pallas as pl
from jax.experimental.pallas import tpu as pltpu
from jax.sharding import PartitionSpec as P

NT = (((1,), (1,)), ((), ()))
TN = (((0,), (0,)), ((), ()))
MESH = pl.DeviceIdType.MESH
VMEM_LIMIT = 64 * 1024 * 1024 - 65536
BF = jnp.bfloat16
ROWS = 256
HALF = ROWS // 2
WIDE = 512


def dot(a, b, dims):
    return lax.dot_general(a, b, dims, preferred_element_type=jnp.float32)


def kernel(
    x, dy, gate, up, wg, wu, wd,
    dxt, dwg, dwu, hid, dgu,
    wd_v, w_v, dy_v, g_v, u_v, dgu_v, h_v, term_v, s_v, q_v, blk_v,
    wd_sem, w_sem, in_sem, out_sem, x_sem, blk_sem, o_sem,
    give_send, give_recv, link_send, link_recv, fin_local, fin_send, fin_recv,
):
    tokens, d = x.shape
    ff = gate.shape[1]
    chunks = tokens // ROWS
    me = lax.axis_index("tp")
    core = lax.rem(me, 2)
    mate = {"tp": me + 1 - 2 * core}
    across = {"tp": lax.rem(me + 2, 4)}
    own = pl.ds(pl.multiple_of(core * HALF, HALF), HALF)
    other = pl.ds(pl.multiple_of((1 - core) * HALF, HALF), HALF)

    def rows_of(c):
        return pl.ds(pl.multiple_of(c * ROWS, ROWS), ROWS)

    def inputs(c):
        r = rows_of(c)
        return (
            pltpu.make_async_copy(dy.at[r, :], dy_v, in_sem.at[0]),
            pltpu.make_async_copy(gate.at[r, :], g_v, in_sem.at[1]),
            pltpu.make_async_copy(up.at[r, :], u_v, in_sem.at[2]),
        )

    def outputs(c):
        r = rows_of(c)
        return (
            pltpu.make_async_copy(dgu_v, dgu.at[r, :], out_sem.at[0]),
            pltpu.make_async_copy(h_v, hid.at[r, :], out_sem.at[1]),
        )

    def wd_piece(j):
        r = pl.ds(j * WIDE, WIDE)
        return pltpu.make_async_copy(wd.at[r, :], wd_v.at[r, :], wd_sem.at[j])

    def w_piece(j):
        r = pl.ds(j * WIDE, WIDE)
        return (
            pltpu.make_async_copy(wg.at[r, :], w_v.at[r, pl.ds(0, ff)], w_sem.at[0, j]),
            pltpu.make_async_copy(wu.at[r, :], w_v.at[r, pl.ds(ff, ff)], w_sem.at[1, j]),
        )

    def give(c):
        return pltpu.make_async_remote_copy(
            term_v.at[other, :], s_v.at[c], give_send.at[c], give_recv.at[c], device_id=mate, device_id_type=MESH
        )

    def link(c):
        return pltpu.make_async_remote_copy(
            s_v.at[c], q_v.at[c], link_send.at[c], link_recv.at[c], device_id=across, device_id_type=MESH
        )

    def final_rows(c):
        return dxt.at[pl.ds(pl.multiple_of(c * ROWS + core * HALF, HALF), HALF), :]

    def fin_here(c):
        return pltpu.make_async_copy(q_v.at[c], final_rows(c), fin_local.at[c])

    def fin_mate(c):
        return pltpu.make_async_remote_copy(
            q_v.at[c], final_rows(c), fin_send.at[c], fin_recv.at[c], device_id=mate, device_id_type=MESH
        )

    def add_term(c):
        give(c).wait_recv()

        def body(i, _):
            r = pl.ds(pl.multiple_of(i * 16, 16), 16)
            mine = term_v[pl.ds(pl.multiple_of(core * HALF + i * 16, 16), 16), :]
            s_v[c, r, :] = (s_v[c, r, :].astype(jnp.float32) + mine.astype(jnp.float32)).astype(BF)
            return 0

        lax.fori_loop(0, HALF // 16, body, 0, unroll=True)
        link(c).start()
        give(c).wait_send()

    def finish(c):
        link(c).wait_recv()

        def body(i, _):
            r = pl.ds(pl.multiple_of(i * 16, 16), 16)
            q_v[c, r, :] = (q_v[c, r, :].astype(jnp.float32) + s_v[c, r, :].astype(jnp.float32)).astype(BF)
            return 0

        lax.fori_loop(0, HALF // 16, body, 0, unroll=True)
        fin_here(c).start()
        fin_mate(c).start()

    def hidden_tile(j):
        cols = pl.ds(j * WIDE, WIDE)
        dh = dot(dy_v[...], wd_v[cols, :], NT)
        g = g_v[:, cols].astype(jnp.float32)
        u = u_v[:, cols].astype(jnp.float32)
        sig = 1.0 / (1.0 + jnp.exp(-g))
        silu = g * sig
        h_v[:, cols] = (silu * u).astype(BF)
        dgu_v[:, pl.ds(ff + j * WIDE, WIDE)] = (dh * silu).astype(BF)
        dgu_v[:, cols] = (dh * u * (sig + silu * (1.0 - sig))).astype(BF)

    def term_tile(j):
        cols = pl.ds(j * WIDE, WIDE)
        term_v[:, cols] = dot(dgu_v[...], w_v[cols, :], NT).astype(BF)

    n_h, n_t = ff // WIDE, d // WIDE

    for cp in inputs(0):
        cp.start()
    for j in range(n_h):
        wd_piece(j).start()
    for j in range(n_t):
        for cp in w_piece(j):
            cp.start()
    barrier = pltpu.get_barrier_semaphore()
    for peer in (mate, across):
        pl.semaphore_signal(barrier, inc=1, device_id=peer, device_id_type=MESH)
    for cp in inputs(0):
        cp.wait()
    for j in range(n_h):
        wd_piece(j).wait()
        hidden_tile(j)
    for cp in inputs(1):
        cp.start()
    for cp in outputs(0):
        cp.start()
    for j in range(n_t):
        for cp in w_piece(j):
            cp.wait()
        term_tile(j)
    pl.semaphore_wait(barrier, 2)
    give(0).start()

    def chunk(c, _):
        for cp in inputs(c):
            cp.wait()
        for cp in outputs(c - 1):
            cp.wait()
        for j in range(n_h // 2):
            hidden_tile(j)
        add_term(c - 1)
        for j in range(n_h // 2, n_h):
            hidden_tile(j)

        @pl.when(c < chunks - 1)
        def _():
            for cp in inputs(c + 1):
                cp.start()

        @pl.when(c == chunks - 1)
        def _():
            pltpu.make_async_copy(x, wd_v, x_sem).start()

        for cp in outputs(c):
            cp.start()

        @pl.when(c >= 5)
        def _():
            finish(c - 5)

        for j in range(n_t):
            term_tile(j)
        give(c).start()
        return 0

    lax.fori_loop(1, chunks, chunk, 0)

    def block(b, slot):
        return pltpu.make_async_copy(
            dgu.at[:, pl.ds(pl.multiple_of(b * WIDE, WIDE), WIDE)], blk_v.at[slot], blk_sem.at[slot]
        )

    tall = 1024
    n_m = d // tall
    n_b = ff // WIDE

    def stage(m, slot):
        return w_v.at[pl.ds(m * tall, tall), pl.ds(pl.multiple_of(slot * WIDE, WIDE), WIDE)]

    def store(m, slot, out, b):
        return pltpu.make_async_copy(
            stage(m, slot),
            out.at[pl.ds(m * tall, tall), pl.ds(pl.multiple_of(b * WIDE, WIDE), WIDE)],
            o_sem.at[slot, m],
        )

    for cp in outputs(chunks - 1):
        cp.wait()
    block(0, 0).start()
    block(1, 1).start()
    pltpu.make_async_copy(x, wd_v, x_sem).wait()

    def column_block(b, _):
        slot = lax.rem(b, 2)

        @pl.when(b == 0)
        def _():
            finish(3)

        @pl.when(b == 1)
        def _():
            add_term(chunks - 1)

        @pl.when(b == 2)
        def _():
            finish(4)

        @pl.when(b == 5)
        def _():
            finish(5)

        @pl.when(b == 7)
        def _():
            finish(6)

        @pl.when(b > 1)
        def _():
            for m in range(n_m):
                store(m, slot, dwg, 0).wait()

        block(b, slot).wait()
        for m in range(n_m):
            stage(m, slot)[...] = dot(wd_v[:, m * tall:(m + 1) * tall], blk_v[slot], TN).astype(BF)

        @pl.when(b < n_b)
        def _():
            for m in range(n_m):
                store(m, slot, dwg, b).start()

        @pl.when(b >= n_b)
        def _():
            for m in range(n_m):
                store(m, slot, dwu, b - n_b).start()

        @pl.when(b < 2 * n_b - 2)
        def _():
            block(b + 2, slot).start()

        return 0

    lax.fori_loop(0, 2 * n_b, column_block, 0)
    finish(chunks - 1)
    for slot in range(2):
        for m in range(n_m):
            store(m, slot, dwg, 0).wait()
    for c in range(chunks):
        link(c).wait_send()
        fin_here(c).wait()
        fin_mate(c).wait()


def last_kernel(
    hid, dy, dxt, dwg_t, dwu_t,
    dx, dwg, dwu, dwd,
    hid_v, dy_v, o_v, cx_v, cg_v, cu_v,
    hid_sem, dy_sem, o_sem, in_sem, out_sem,
):
    tokens, ff = hid.shape
    d = dy.shape[1]
    steps = d // WIDE
    tall = ff // 2
    strip = dwg.shape[0] // steps

    def cols(n):
        return pl.ds(pl.multiple_of(n * WIDE, WIDE), WIDE)

    def strip_of(n):
        return pl.ds(pl.multiple_of(n * strip, strip), strip)

    def load_hid(m):
        c = pl.ds(m * tall, tall)
        return pltpu.make_async_copy(hid.at[:, c], hid_v.at[:, c], hid_sem.at[m])

    def load_dy(n, slot):
        return pltpu.make_async_copy(dy.at[:, cols(n)], dy_v.at[slot], dy_sem.at[slot])

    def take(n, slot):
        return (
            pltpu.make_async_copy(dxt.at[:, cols(n)], cx_v.at[slot], in_sem.at[slot, 0]),
            pltpu.make_async_copy(dwg_t.at[strip_of(n), :], cg_v.at[slot], in_sem.at[slot, 1]),
            pltpu.make_async_copy(dwu_t.at[strip_of(n), :], cu_v.at[slot], in_sem.at[slot, 2]),
        )

    def put(n, slot):
        return (
            pltpu.make_async_copy(cx_v.at[slot], dx.at[:, cols(n)], out_sem.at[slot, 0]),
            pltpu.make_async_copy(cg_v.at[slot], dwg.at[strip_of(n), :], out_sem.at[slot, 1]),
            pltpu.make_async_copy(cu_v.at[slot], dwu.at[strip_of(n), :], out_sem.at[slot, 2]),
        )

    def store(m, n, slot):
        return pltpu.make_async_copy(
            o_v.at[slot, m], dwd.at[pl.ds(m * tall, tall), cols(n)], o_sem.at[slot, m]
        )

    load_hid(0).start()
    load_dy(0, 0).start()
    load_hid(1).start()
    load_dy(1, 1).start()
    for cp in take(0, 0):
        cp.start()
    load_hid(0).wait()
    load_hid(1).wait()

    def column_block(n, _):
        slot = lax.rem(n, 2)

        @pl.when(n > 1)
        def _():
            for m in range(2):
                store(m, n, slot).wait()

        @pl.when(n > 0)
        def _():
            for cp in put(n - 1, 1 - slot):
                cp.wait()

        @pl.when(n < steps - 1)
        def _():
            for cp in take(n + 1, 1 - slot):
                cp.start()

        load_dy(n, slot).wait()
        for cp in take(n, slot):
            cp.wait()
        for cp in put(n, slot):
            cp.start()
        for m in range(2):
            o_v[slot, m] = dot(hid_v[:, m * tall:(m + 1) * tall], dy_v[slot], TN).astype(BF)
        for m in range(2):
            store(m, n, slot).start()

        @pl.when(n < steps - 2)
        def _():
            load_dy(n + 2, slot).start()

        return 0

    lax.fori_loop(0, steps, column_block, 0)
    for cp in put(steps - 1, (steps - 1) % 2):
        cp.wait()
    for slot in range(2):
        for m in range(2):
            store(m, 0, slot).wait()


def solution(mesh):
    def step(x, dy, gate, up, w_gate, w_up, w_down):
        tokens, d = x.shape
        ff = gate.shape[1]
        chunks = tokens // ROWS
        hbm = pl.BlockSpec(memory_space=pl.ANY)
        dma = pltpu.SemaphoreType.DMA
        dxt, dwg, dwu, hid, _ = pl.pallas_call(
            kernel,
            name="chunks",
            in_specs=[hbm] * 7,
            out_specs=[hbm] * 5,
            out_shape=[
                jax.ShapeDtypeStruct((tokens, d), BF),
                jax.ShapeDtypeStruct((d, ff), BF),
                jax.ShapeDtypeStruct((d, ff), BF),
                jax.ShapeDtypeStruct((tokens, ff), BF),
                jax.ShapeDtypeStruct((tokens, 2 * ff), BF),
            ],
            scratch_shapes=[
                pltpu.VMEM((ff, d), BF),
                pltpu.VMEM((d, 2 * ff), BF),
                pltpu.VMEM((ROWS, d), BF),
                pltpu.VMEM((ROWS, ff), BF),
                pltpu.VMEM((ROWS, ff), BF),
                pltpu.VMEM((ROWS, 2 * ff), BF),
                pltpu.VMEM((ROWS, ff), BF),
                pltpu.VMEM((ROWS, d), BF),
                pltpu.VMEM((chunks, HALF, d), BF),
                pltpu.VMEM((chunks, HALF, d), BF),
                pltpu.VMEM((2, tokens, WIDE), BF),
                dma((ff // WIDE,)),
                dma((2, d // WIDE)),
                dma((3,)),
                dma((2,)),
                dma,
                dma((2,)),
                dma((2, d // 1024)),
            ]
            + [dma((chunks,))] * 7,
            compiler_params=pltpu.CompilerParams(
                collective_id=0, has_side_effects=True, vmem_limit_bytes=VMEM_LIMIT
            ),
        )(x, dy, gate, up, w_gate, w_up, w_down)
        strip = d // (d // WIDE)
        return pl.pallas_call(
            last_kernel,
            name="down",
            in_specs=[hbm] * 5,
            out_specs=[hbm] * 4,
            out_shape=[
                jax.ShapeDtypeStruct((tokens, d), BF),
                jax.ShapeDtypeStruct((d, ff), BF),
                jax.ShapeDtypeStruct((d, ff), BF),
                jax.ShapeDtypeStruct((ff, d), BF),
            ],
            scratch_shapes=[
                pltpu.VMEM((tokens, ff), BF),
                pltpu.VMEM((2, tokens, WIDE), BF),
                pltpu.VMEM((2, 2, ff // 2, WIDE), BF),
                pltpu.VMEM((2, tokens, WIDE), BF),
                pltpu.VMEM((2, strip, ff), BF),
                pltpu.VMEM((2, strip, ff), BF),
                dma((2,)),
                dma((2,)),
                dma((2, 2)),
                dma((2, 3)),
                dma((2, 3)),
            ],
            compiler_params=pltpu.CompilerParams(vmem_limit_bytes=VMEM_LIMIT),
        )(hid, dy, dxt, dwg, dwu)

    tokens, columns, rows = P("dp", None), P(None, "tp"), P("tp", None)
    return jax.shard_map(
        step,
        mesh=mesh,
        in_specs=(tokens, tokens, P("dp", "tp"), P("dp", "tp"), columns, columns, rows),
        out_specs=(tokens, P("dp", "tp"), P("dp", "tp"), P(("dp", "tp"), None)),
        check_vma=False,
    )
```
